32 devices in a mesh: rep: 4 (over y, core), row: 4 (over z), col: 2 (over x).
Axes of the slice: x: 2, y: 2, z: 4, core: 2. Of those that a mesh axis runs over, the one named last changes fastest.
Arguments:
- patches: bfloat16 [4096, 588], P(('rep', 'col')), may hold values from -20 to 20
- embed_weight: bfloat16 [588, 6144], P(None, 'row'), may hold values from -1 to 1
- embed_bias: float32 [6144], P('row'), may hold values from -3 to 3
- old_in: bfloat16 [64, 768, 1536], P(('row', 'col')), may hold values from -0.078125 to 0.078125
- old_out: bfloat16 [64, 1536, 768], P(('row', 'col')), may hold values from -0.0546875 to 0.0546875
- restore_id: int32 [1], replicated, may hold values from 0 to 47
- norm_gains: float32 [48, 6144], P(None, 'row'), may hold values from 0.1 to 1.9
- in_biases: float32 [48, 12288], P(None, 'col'), may hold values from -3 to 3
- out_biases: float32 [48, 6144], P(None, 'row'), may hold values from -3 to 3
- final_gain: float32 [6144], P('row'), may hold values from 0.1 to 1.9
- check_weight: bfloat16 [6144, 128], P('row'), may hold values from -0.078125 to 0.078125
Outputs:
- in_weight: bfloat16 [6144, 12288], P('row', 'col')
- out_weight: bfloat16 [12288, 6144], P('col', 'row')
- check_logits: float32 [4096, 128], P(('rep', 'col'))
The draws below stay inside these ranges and needn't reach their ends.
All inputs are finite; a program needn't handle non-finite values.
Results may differ from the reference program's by a relative error of at most 0.0062.
Values may be sent and summed in bfloat16 or wider, within the bound.
A program may use at most 192 MiB of HBM per device.

```python
import math
import jax
import jax.numpy as jnp
from jax import lax

D = 6144
PATCH = 588
LAYERS_ALL = 48
FF = 12288
OLD_GRID = 8
CHECK = 128
TOKENS = 4096


def draw_patches(key, part):
    base_key, scale_key = jax.random.split(key, 2)
    row_scale = jnp.exp(jax.random.uniform(scale_key, (TOKENS, 1), jnp.float32, math.log(0.5), math.log(5.0)))
    noise_part = jax.random.truncated_normal(base_key, -4.0, 4.0, (TOKENS, PATCH), jnp.float32)
    values = row_scale * noise_part
    return values.astype(jnp.bfloat16)


def draw_embed_weight(key, part):
    entry_key, column_key = jax.random.split(key, 2)
    position = jnp.arange(D, dtype=jnp.float32) / D
    trend_part = math.log(3.0) * (position - 0.5)
    jitter = jax.random.uniform(column_key, (D,), jnp.float32, -1.15, 1.15)
    entries = jax.random.truncated_normal(entry_key, -4.0, 4.0, (PATCH, D), jnp.float32)
    column_scale = jnp.exp(trend_part + jitter)
    return (entries * column_scale[None, :] / math.sqrt(PATCH)).astype(jnp.bfloat16)


def block_levels(key, extent, cuts, smallest, largest):
    factor_of, own = 1.0, jax.random.fold_in(key, 6)
    for dim, parts in cuts:
        draws = jnp.exp(jax.random.uniform(jax.random.fold_in(own, dim), (parts,), jnp.float32, smallest / len(cuts), largest / len(cuts)))
        factor_of = factor_of * jnp.repeat(draws, extent[dim] // parts).reshape([-1 if axis == dim else 1 for axis in range(len(extent))])
    return factor_of


def normal_values(rng, extent, deviation, reach, cuts=(), held_as=jnp.bfloat16):
    values = jax.random.normal(rng, extent, jnp.float32) * deviation
    if len(cuts) > 0:
        values = block_levels(rng, extent, cuts, -0.22, 0.18) * values
    return jnp.clip(values, min=-reach, max=reach).astype(held_as)


def setup_inputs(seed: int = 0) -> dict:
    key_of = jax.random.split(jax.random.key(seed), 12)
    return {
        "patches": draw_patches(jax.random.fold_in(key_of[11], 71), 0),
        "embed_weight": draw_embed_weight(jax.random.fold_in(key_of[11], 71), 0),
        "embed_bias": normal_values(key_of[2], (D,), 0.5, 3.0, ((0, 4),), jnp.float32),
        "old_in": normal_values(key_of[3], (OLD_GRID * OLD_GRID, D // OLD_GRID, FF // OLD_GRID), D ** -0.5, 0.078125, ((0, 8),)),
        "old_out": normal_values(key_of[4], (OLD_GRID * OLD_GRID, FF // OLD_GRID, D // OLD_GRID), FF ** -0.5, 0.0546875, ((0, 8),)),
        "restore_id": jax.random.randint(key_of[5], (1,), 0, LAYERS_ALL).astype(jnp.int32),
        "norm_gains": jnp.clip(1.0 + 0.18 * jax.random.normal(key_of[6], (LAYERS_ALL, D), jnp.float32), 0.1, 1.9),
        "in_biases": normal_values(key_of[7], (LAYERS_ALL, FF), 0.5, 3.0, ((1, 2),), jnp.float32),
        "out_biases": normal_values(key_of[8], (LAYERS_ALL, D), 0.5, 3.0, ((1, 4),), jnp.float32),
        "final_gain": jnp.clip(1.0 + 0.18 * jax.random.normal(key_of[9], (D,), jnp.float32), 0.1, 1.9),
        "check_weight": normal_values(key_of[10], (D, CHECK), D ** -0.5, 0.078125, ((0, 4),)),
    }


EPSILON = 1e-06

def assemble_in(old_tiles):
    tile_grid = old_tiles.reshape(OLD_GRID, OLD_GRID, D // OLD_GRID, FF // OLD_GRID)
    return tile_grid.transpose(0, 2, 1, 3).reshape(D, FF)

def assemble_out(old_tiles):
    tile_grid = old_tiles.reshape(OLD_GRID, OLD_GRID, FF // OLD_GRID, D // OLD_GRID)
    return tile_grid.transpose(1, 2, 0, 3).reshape(FF, D)

def pick_rows(restore_id, param_table):
    selector = (jnp.arange(param_table.shape[0], dtype=jnp.int32)[None, :] == restore_id[:, None]).astype(jnp.float32)
    return jnp.dot(selector, param_table, precision=lax.Precision.HIGHEST)[0]

def norm_rows(values, gain_row):
    feature_count = values.shape[1]
    average = lax.optimization_barrier(jnp.sum(values, axis=1, keepdims=True)) / feature_count
    square_mean = lax.optimization_barrier(jnp.sum(values * values, axis=1, keepdims=True)) / feature_count
    inverse_scale = lax.rsqrt(square_mean - average * average + EPSILON)
    return ((values - average) * inverse_scale * gain_row).astype(jnp.bfloat16)

def reference(patches, embed_weight, embed_bias, old_in, old_out, restore_id, norm_gains, in_biases, out_biases, final_gain, check_weight):
    in_weight = assemble_in(old_in)
    out_weight = assemble_out(old_out)
    layer_gain = pick_rows(restore_id, norm_gains)
    layer_in_bias = pick_rows(restore_id, in_biases)
    layer_out_bias = pick_rows(restore_id, out_biases)
    embedded = jnp.dot(patches, embed_weight, preferred_element_type=jnp.float32) + embed_bias
    normed = norm_rows(embedded, layer_gain)
    pre = jnp.dot(normed, in_weight, preferred_element_type=jnp.float32) + layer_in_bias
    hidden = jax.nn.gelu(pre, approximate=False).astype(jnp.bfloat16)
    updated = embedded + jnp.dot(hidden, out_weight, preferred_element_type=jnp.float32) + layer_out_bias
    final_normed = norm_rows(updated, final_gain)
    check_logits = jnp.dot(final_normed, check_weight, preferred_element_type=jnp.float32)
    return (in_weight, out_weight, check_logits)
```

```python
import functools

import jax
import jax.numpy as jnp
from jax import lax
from jax.experimental import pallas as pl
from jax.experimental.pallas import tpu as pltpu
from jax.sharding import PartitionSpec as P

EPSILON = 1e-06
CHUNKS = 2


def for_sending(shard):
    return jax.tree.map(lambda a: a.astype(jnp.bfloat16) if a.dtype == jnp.float32 else a, shard)


def partner(value, axis, bit):
    mask = 2**bit
    pairs = [(source, source ^ mask) for source in range(lax.axis_size(axis))]
    return lax.ppermute(value, axis, pairs)


def pick_rows(restore_id, param_table):
    selector = (
        jnp.arange(param_table.shape[0], dtype=jnp.int32)[None, :] == restore_id[:, None]
    ).astype(jnp.float32)
    return jnp.dot(selector, param_table, precision=lax.Precision.HIGHEST)[0]


def norm_rows(values, gain_row):
    feature_count = values.shape[1] * lax.axis_size("row")
    totals = lax.psum((jnp.sum(values, axis=1), jnp.sum(values * values, axis=1)), "row")
    average = totals[0][:, None] / feature_count
    spread = totals[1][:, None] / feature_count - average * average
    return ((values - average) * lax.rsqrt(spread + EPSILON) * gain_row).astype(jnp.bfloat16)


def move_halves(pieces, bit_total, device_index, exchange):
    for bit_number in range(bit_total):
        upper_side = device_index >> bit_number & 1 == 1
        outgoing = tuple(
            (jnp.where(upper_side, lower_part, upper_part) for lower_part, upper_part in pieces)
        )
        incoming = exchange(outgoing, bit_number)
        pieces = tuple(
            (
                (
                    jnp.where(upper_side, arrived, lower_part),
                    jnp.where(upper_side, upper_part, arrived),
                )
                for (lower_part, upper_part), arrived in zip(pieces, incoming)
            )
        )
    return pieces


def butterfly_weights(old_in, old_out):
    tiles_here, tile_rows, tile_cols = old_in.shape
    local_cols = tiles_here * tile_cols
    half_cols = local_cols // 2
    in_local = jnp.transpose(old_in, (1, 0, 2)).reshape(tile_rows, local_cols)
    out_local = old_out.reshape(local_cols, tile_rows)
    col_index = lax.axis_index("col")
    col_count = lax.axis_size("col")
    col_bits = col_count.bit_length() - 1
    pieces = (
        (in_local[:, :half_cols], in_local[:, half_cols:]),
        (out_local[:half_cols], out_local[half_cols:]),
    )
    pieces = move_halves(
        pieces,
        col_bits,
        col_index,
        lambda send_parts, bit_number: jax.tree.map(
            lambda part, own: part.astype(own.dtype),
            partner(for_sending(send_parts), "col", bit_number),
            send_parts,
        ),
    )
    in_pair, out_pair = pieces
    in_weight = jnp.concatenate(in_pair, axis=0)
    out_weight = jnp.concatenate(out_pair, axis=1)
    return in_weight, out_weight


def shared_exchange(old_in, old_out):
    tiles_here, tile_rows, tile_cols = old_in.shape
    half_tiles = tiles_here // 2
    half_cols = half_tiles * tile_cols
    col_index = lax.axis_index("col")
    rep_index = lax.axis_index("rep")
    rep_count = lax.axis_size("rep")
    in_parts = old_in.reshape(2, rep_count, half_tiles * tile_rows // rep_count, tile_cols)
    share = lax.dynamic_slice(
        in_parts, (1 - col_index, rep_index, 0, 0), (1, 1) + in_parts.shape[2:]
    )[0, 0]
    share = partner(share, "col", 0)
    out_parts = old_out.reshape(2, half_cols, tile_rows)
    out_sent = lax.dynamic_index_in_dim(out_parts, 1 - col_index, 0, keepdims=False)
    out_kept = lax.dynamic_index_in_dim(out_parts, col_index, 0, keepdims=False)
    share, out_sent = lax.optimization_barrier((share, out_sent))
    out_arrived = partner(out_sent, "col", 0)
    in_arrived = lax.all_gather(share, "rep", axis=0, tiled=True)

    def as_rows(tiles):
        rows = tiles.reshape(half_tiles, tile_rows, tile_cols)
        return jnp.transpose(rows, (1, 0, 2)).reshape(1, tile_rows, half_cols)

    kept = as_rows(lax.dynamic_index_in_dim(in_parts, col_index, 0, keepdims=False))
    blocks = jnp.zeros((2, tile_rows, half_cols), old_in.dtype)
    blocks = lax.dynamic_update_slice(blocks, kept, (col_index, 0, 0))
    blocks = lax.dynamic_update_slice(blocks, as_rows(in_arrived), (1 - col_index, 0, 0))
    return blocks.reshape(2 * tile_rows, half_cols), out_kept, out_arrived


def join_out(out_kept, out_arrived):
    upper_side = lax.axis_index("col") == 1
    return jnp.concatenate(
        (
            jnp.where(upper_side, out_arrived, out_kept),
            jnp.where(upper_side, out_kept, out_arrived),
        ),
        axis=1,
    )


def on_device(
    patches,
    embed_weight,
    embed_bias,
    old_in,
    old_out,
    restore_id,
    norm_gains,
    in_biases,
    out_biases,
    final_gain,
    check_weight,
):
    paired = (
        lax.axis_size("col") == 2
        and old_in.shape[0] % 2 == 0
        and (old_in.shape[0] // 2 * old_in.shape[1]) % lax.axis_size("rep") == 0
    )
    if paired:
        in_weight, out_kept, out_arrived = shared_exchange(old_in, old_out)
    else:
        in_weight, out_weight = butterfly_weights(old_in, old_out)
    layer_gain = pick_rows(restore_id, norm_gains)
    in_bias = pick_rows(restore_id, in_biases)
    out_bias = pick_rows(restore_id, out_biases)
    embedded = jnp.dot(patches, embed_weight, preferred_element_type=jnp.float32) + embed_bias
    normed = norm_rows(embedded, layer_gain)
    tokens = lax.all_gather(normed, "col", axis=0, tiled=True)
    chunk_rows = tokens.shape[0] // CHUNKS
    pre_shares = []
    for chunk in range(CHUNKS):
        partial_pre = jnp.dot(
            tokens[chunk * chunk_rows : (chunk + 1) * chunk_rows],
            in_weight,
            preferred_element_type=jnp.float32,
        ).astype(jnp.bfloat16)
        pre_shares.append(
            lax.psum_scatter(partial_pre, "row", scatter_dimension=0, tiled=True)
        )
    hidden_chunks = [
        jax.nn.gelu(share.astype(jnp.float32) + in_bias, approximate=False).astype(jnp.bfloat16)
        for share in pre_shares
    ]
    if paired:
        hidden_chunks[0], out_arrived = lax.optimization_barrier((hidden_chunks[0], out_arrived))
        out_weight = join_out(out_kept, out_arrived)
    partial_branch = jnp.concatenate(
        [
            jnp.dot(
                lax.all_gather(hidden, "row", axis=0, tiled=True),
                out_weight,
                preferred_element_type=jnp.float32,
            ).astype(jnp.bfloat16)
            for hidden in hidden_chunks
        ],
        axis=0,
    )
    updated = (
        embedded
        + lax.psum_scatter(partial_branch, "col", scatter_dimension=0, tiled=True).astype(jnp.float32)
        + out_bias
    )
    final_normed = norm_rows(updated, final_gain)
    check_logits = lax.psum(
        jnp.dot(final_normed, check_weight, preferred_element_type=jnp.float32), "row"
    )
    return (in_weight, out_weight, check_logits)

TAIL_LOG2 = (
    -0.9999999403953552,
    -1.1511064767837524,
    -0.4591980278491974,
    -0.05252550542354584,
    0.0070996368303895,
    -0.00015319570957217366,
    -0.00018990339594893157,
    4.5312575821299106e-05,
    -4.725873623101506e-06,
    1.9546290275229694e-07,
)
TAIL_END = 6.0


def exact_gelu(value):
    size = jnp.abs(value)
    at = jnp.minimum(size, TAIL_END)
    power = TAIL_LOG2[-1]
    for coefficient in TAIL_LOG2[-2::-1]:
        power = power * at + coefficient
    return jnp.maximum(value, 0.0) - size * jnp.exp2(power)


def branch_kernel(blocks, tok_ref, scale_ref, map_ref, bias_ref, weight_ref, out_ref, total, held):
    step = pl.program_id(0)

    @pl.when(step == 0)
    def _():
        total[...] = jnp.zeros_like(total)
        held[...] = jnp.zeros_like(held)

    total[...] += jnp.dot(held[...], weight_ref[...], preferred_element_type=jnp.float32)
    pre = jnp.dot(tok_ref[...], map_ref[0], preferred_element_type=jnp.float32)
    held[...] = exact_gelu(pre * scale_ref[...] + bias_ref[...]).astype(held.dtype)

    @pl.when(step == blocks)
    def _():
        out_ref[...] = total[...].astype(out_ref.dtype)


def branch(tok, scale, maps, in_bias, out_weight, out_type, block):
    rows, depth = tok.shape
    groups, _, group_cols = maps.shape
    hidden_count, features = out_weight.shape
    blocks = hidden_count // block
    per_group = group_cols // block

    def now(step):
        return jnp.minimum(step, blocks - 1)

    def before(step):
        return jnp.maximum(step - 1, 0)

    return pl.pallas_call(
        functools.partial(branch_kernel, blocks),
        grid=(blocks + 1,),
        out_shape=jax.ShapeDtypeStruct((rows, features), out_type),
        in_specs=[
            pl.BlockSpec((rows, depth), lambda i: (0, 0)),
            pl.BlockSpec((rows, 1), lambda i: (0, 0)),
            pl.BlockSpec((1, depth, block), lambda i: (now(i) // per_group, 0, now(i) % per_group)),
            pl.BlockSpec((1, block), lambda i: (0, now(i))),
            pl.BlockSpec((block, features), lambda i: (before(i), 0)),
        ],
        out_specs=pl.BlockSpec((rows, features), lambda i: (0, 0)),
        scratch_shapes=[
            pltpu.VMEM((rows, features), jnp.float32),
            pltpu.VMEM((rows, block), jnp.bfloat16),
        ],
        compiler_params=pltpu.CompilerParams(vmem_limit_bytes=48 * 2**20),
        cost_estimate=pl.CostEstimate(
            flops=2 * rows * hidden_count * (depth + features),
            bytes_accessed=2 * hidden_count * (depth + features),
            transcendentals=rows * hidden_count,
        ),
        name="branch",
    )(tok, scale, maps, in_bias[None, :], out_weight)


def place_kernel(axis, count, place_ref, own_ref, *refs):
    arrived, out_ref = refs[:-1], refs[-1]
    col = place_ref[0]
    extent = own_ref.shape[1 + axis]
    step = pl.program_id(0)

    def window(index):
        start = pl.multiple_of(index * extent, 128)
        return (pl.ds(start, extent), slice(None)) if axis == 0 else (slice(None), pl.ds(start, extent))

    out_ref[window(col)] = own_ref[0]
    for number in range(count):
        @pl.when(step == number)
        def _(number=number):
            out_ref[window(1 - col)] = arrived[number][...]


def place_tiles(old, arrived, axis):
    count = len(arrived)
    _, rows, cols = old.shape
    place = jnp.stack([lax.axis_index("col"), lax.axis_index("rep")]).astype(jnp.int32)
    if axis == 0:
        out_shape, out_block = (2 * rows, count * cols), (2 * rows, cols)
        out_map = lambda i, place: (0, place[1] ^ i)
    else:
        out_shape, out_block = (count * rows, 2 * cols), (rows, 2 * cols)
        out_map = lambda i, place: (place[1] ^ i, 0)
    return pl.pallas_call(
        functools.partial(place_kernel, axis, count),
        grid_spec=pltpu.PrefetchScalarGridSpec(
            num_scalar_prefetch=1,
            grid=(count,),
            in_specs=[pl.BlockSpec((1, rows, cols), lambda i, place: (place[0] * count + (place[1] ^ i), 0, 0))]
            + [pl.BlockSpec((rows, cols), lambda i, place: (0, 0))] * count,
            out_specs=pl.BlockSpec(out_block, out_map),
        ),
        out_shape=jax.ShapeDtypeStruct(out_shape, old.dtype),
        compiler_params=pltpu.CompilerParams(vmem_limit_bytes=56 * 2**20),
        cost_estimate=pl.CostEstimate(
            flops=2 * rows * cols * count * 4096, bytes_accessed=8 * rows * cols * count, transcendentals=0
        ),
        name="place",
    )(place, old, *arrived)


def rep_partner(value, mask):
    return lax.ppermute(value, "rep", [(s, s ^ mask) for s in range(lax.axis_size("rep"))])


def after(value, *others):
    return lax.optimization_barrier((value,) + others)[0]


def spread_over_rep(share, first):
    across = rep_partner(share, 2)
    return (share, rep_partner(share, 1), across, rep_partner(across, 1))


def row_of(restore_id, table):
    return lax.dynamic_slice_in_dim(table, restore_id[0], 1, axis=0)[0]


def fast_device(
    patches,
    embed_weight,
    embed_bias,
    old_in,
    old_out,
    restore_id,
    norm_gains,
    in_biases,
    out_biases,
    final_gain,
    check_weight,
):
    col, rep = lax.axis_index("col"), lax.axis_index("rep")
    rep_count, row_count = lax.axis_size("rep"), lax.axis_size("row")
    tile_rows = old_in.shape[1]
    token_count, patch_size = patches.shape
    feature_count = embed_weight.shape[1] * row_count
    depth = -(-(patch_size + 1) // (32 * row_count)) * 32 * row_count

    layer_gain = row_of(restore_id, norm_gains)
    in_bias = row_of(restore_id, in_biases)
    out_bias = row_of(restore_id, out_biases)

    def tile(old, half):
        return lax.dynamic_index_in_dim(old, half * rep_count + rep, 0, keepdims=False)

    in_share = partner(tile(old_in, 1 - col), "col", 0)
    embedded = jnp.dot(patches, embed_weight, preferred_element_type=jnp.float32) + embed_bias
    weights32 = embed_weight.astype(jnp.float32)
    check32 = check_weight.astype(jnp.float32) * final_gain[:, None]
    sums = lax.psum(
        (
            jnp.sum(embedded, axis=1),
            jnp.sum(embedded * embedded, axis=1),
            jnp.sum(weights32, axis=1),
            jnp.sum(embed_bias)[None],
            jnp.sum(check32, axis=0),
        ),
        "row",
    )
    average = sums[0] / feature_count
    scale = lax.rsqrt(sums[1] / feature_count - average * average + EPSILON)
    weight_mean, bias_mean, check_sum = sums[2] / feature_count, sums[3] / feature_count, sums[4]

    lifted = jnp.concatenate(
        (
            (weights32 - weight_mean[:, None]) * layer_gain,
            ((embed_bias - bias_mean) * layer_gain)[None, :],
            jnp.zeros((depth - patch_size - 1, embed_weight.shape[1]), jnp.float32),
        ),
        axis=0,
    ).astype(jnp.bfloat16)
    own_part = lax.dynamic_slice_in_dim(lifted, col * tile_rows, tile_rows, axis=1)
    far_part = lax.dynamic_slice_in_dim(lifted, (1 - col) * tile_rows, tile_rows, axis=1)
    near_map = jnp.dot(own_part, tile(old_in, col), preferred_element_type=jnp.float32)
    far_map = jnp.dot(far_part, in_share, preferred_element_type=jnp.float32)
    map_part = (near_map + far_map).astype(jnp.bfloat16)
    map_piece = lax.psum_scatter(map_part, "row", scatter_dimension=0, tiled=True)
    maps = lax.all_gather(map_piece, ("rep", "row"), axis=0, tiled=True)
    maps = maps.reshape(rep_count, depth, old_in.shape[2])

    tok = jnp.concatenate(
        (
            patches,
            jnp.ones((token_count, 1), patches.dtype),
            jnp.zeros((token_count, depth - patch_size - 1), patches.dtype),
        ),
        axis=1,
    )
    patches_sent, scale_sent = after((patches, scale), in_share)
    far_patches = partner(patches_sent, "col", 0)
    far_scale = partner(scale_sent, "col", 0)
    far_tok = jnp.concatenate((far_patches, tok[:, patch_size:]), axis=1)

    out_sent = after(tile(old_out, 1 - col), in_share, far_patches)
    out_share = partner(out_sent, "col", 0)
    out_weight = place_tiles(old_out, spread_over_rep(out_share, 2), 1)
    in_sent = after(in_share, out_share)
    in_weight = place_tiles(old_in, spread_over_rep(in_sent, 2), 0)

    block = 512
    far_total = branch(far_tok, far_scale[:, None], maps, in_bias, out_weight, jnp.bfloat16, block)
    near_tok, far_total = lax.optimization_barrier((tok, far_total))
    arrived = partner(far_total, "col", 0)
    near_total = branch(near_tok, scale[:, None], maps, in_bias, out_weight, jnp.float32, block)
    updated = embedded + near_total + arrived.astype(jnp.float32) + out_bias

    def halves(value):
        upper = lax.reduce_precision(value, 8, 7)
        return upper.astype(jnp.bfloat16), (value - upper).astype(jnp.bfloat16)

    updated_hi, updated_lo = halves(updated)
    check_hi, check_lo = halves(check32)
    raw = (
        jnp.dot(updated_hi, check_hi, preferred_element_type=jnp.float32)
        + jnp.dot(updated_lo, check_hi, preferred_element_type=jnp.float32)
        + jnp.dot(updated_hi, check_lo, preferred_element_type=jnp.float32)
    )
    raw, total, squares = lax.psum(
        (raw, jnp.sum(updated, axis=1), jnp.sum(updated * updated, axis=1)), "row"
    )
    average = (total / feature_count)[:, None]
    spread = (squares / feature_count)[:, None] - average * average
    check_logits = lax.rsqrt(spread + EPSILON) * (raw - average * check_sum)
    return (in_weight, out_weight, check_logits)


def on_either(*args):
    old_in = args[3]
    shared = (
        lax.axis_size("col") == 2
        and lax.axis_size("rep") == 4
        and old_in.shape[0] == 2 * lax.axis_size("rep")
    )
    return fast_device(*args) if shared else on_device(*args)


def solution(mesh):
    placed = (
        P(("rep", "col"), None),
        P(None, "row"),
        P("row"),
        P(("row", "col"), None, None),
        P(("row", "col"), None, None),
        P(),
        P(None, "row"),
        P(None, "col"),
        P(None, "row"),
        P("row"),
        P("row", None),
    )
    return jax.shard_map(
        on_either,
        mesh=mesh,
        in_specs=placed,
        out_specs=(P("row", "col"), P("col", "row"), P(("rep", "col"), None)),
        check_vma=False,
    )
```

```python
import functools

import jax
import jax.numpy as jnp
from jax import lax
from jax.experimental import pallas as pl
from jax.experimental.pallas import tpu as pltpu
from jax.sharding import PartitionSpec as P

EPSILON = 1e-06
CHUNKS = 2


def for_sending(shard):
    return jax.tree.map(lambda a: a.astype(jnp.bfloat16) if a.dtype == jnp.float32 else a, shard)


def partner(value, axis, bit):
    mask = 2**bit
    pairs = [(source, source ^ mask) for source in range(lax.axis_size(axis))]
    return lax.ppermute(value, axis, pairs)


def pick_rows(restore_id, param_table):
    selector = (
        jnp.arange(param_table.shape[0], dtype=jnp.int32)[None, :] == restore_id[:, None]
    ).astype(jnp.float32)
    return jnp.dot(selector, param_table, precision=lax.Precision.HIGHEST)[0]


def norm_rows(values, gain_row):
    feature_count = values.shape[1] * lax.axis_size("row")
    totals = lax.psum((jnp.sum(values, axis=1), jnp.sum(values * values, axis=1)), "row")
    average = totals[0][:, None] / feature_count
    spread = totals[1][:, None] / feature_count - average * average
    return ((values - average) * lax.rsqrt(spread + EPSILON) * gain_row).astype(jnp.bfloat16)


def move_halves(pieces, bit_total, device_index, exchange):
    for bit_number in range(bit_total):
        upper_side = device_index >> bit_number & 1 == 1
        outgoing = tuple(
            (jnp.where(upper_side, lower_part, upper_part) for lower_part, upper_part in pieces)
        )
        incoming = exchange(outgoing, bit_number)
        pieces = tuple(
            (
                (
                    jnp.where(upper_side, arrived, lower_part),
                    jnp.where(upper_side, upper_part, arrived),
                )
                for (lower_part, upper_part), arrived in zip(pieces, incoming)
            )
        )
    return pieces


def butterfly_weights(old_in, old_out):
    tiles_here, tile_rows, tile_cols = old_in.shape
    local_cols = tiles_here * tile_cols
    half_cols = local_cols // 2
    in_local = jnp.transpose(old_in, (1, 0, 2)).reshape(tile_rows, local_cols)
    out_local = old_out.reshape(local_cols, tile_rows)
    col_index = lax.axis_index("col")
    col_count = lax.axis_size("col")
    col_bits = col_count.bit_length() - 1
    pieces = (
        (in_local[:, :half_cols], in_local[:, half_cols:]),
        (out_local[:half_cols], out_local[half_cols:]),
    )
    pieces = move_halves(
        pieces,
        col_bits,
        col_index,
        lambda send_parts, bit_number: jax.tree.map(
            lambda part, own: part.astype(own.dtype),
            partner(for_sending(send_parts), "col", bit_number),
            send_parts,
        ),
    )
    in_pair, out_pair = pieces
    in_weight = jnp.concatenate(in_pair, axis=0)
    out_weight = jnp.concatenate(out_pair, axis=1)
    return in_weight, out_weight


def shared_exchange(old_in, old_out):
    tiles_here, tile_rows, tile_cols = old_in.shape
    half_tiles = tiles_here // 2
    half_cols = half_tiles * tile_cols
    col_index = lax.axis_index("col")
    rep_index = lax.axis_index("rep")
    rep_count = lax.axis_size("rep")
    in_parts = old_in.reshape(2, rep_count, half_tiles * tile_rows // rep_count, tile_cols)
    share = lax.dynamic_slice(
        in_parts, (1 - col_index, rep_index, 0, 0), (1, 1) + in_parts.shape[2:]
    )[0, 0]
    share = partner(share, "col", 0)
    out_parts = old_out.reshape(2, half_cols, tile_rows)
    out_sent = lax.dynamic_index_in_dim(out_parts, 1 - col_index, 0, keepdims=False)
    out_kept = lax.dynamic_index_in_dim(out_parts, col_index, 0, keepdims=False)
    share, out_sent = lax.optimization_barrier((share, out_sent))
    out_arrived = partner(out_sent, "col", 0)
    in_arrived = lax.all_gather(share, "rep", axis=0, tiled=True)

    def as_rows(tiles):
        rows = tiles.reshape(half_tiles, tile_rows, tile_cols)
        return jnp.transpose(rows, (1, 0, 2)).reshape(1, tile_rows, half_cols)

    kept = as_rows(lax.dynamic_index_in_dim(in_parts, col_index, 0, keepdims=False))
    blocks = jnp.zeros((2, tile_rows, half_cols), old_in.dtype)
    blocks = lax.dynamic_update_slice(blocks, kept, (col_index, 0, 0))
    blocks = lax.dynamic_update_slice(blocks, as_rows(in_arrived), (1 - col_index, 0, 0))
    return blocks.reshape(2 * tile_rows, half_cols), out_kept, out_arrived


def join_out(out_kept, out_arrived):
    upper_side = lax.axis_index("col") == 1
    return jnp.concatenate(
        (
            jnp.where(upper_side, out_arrived, out_kept),
            jnp.where(upper_side, out_kept, out_arrived),
        ),
        axis=1,
    )


def on_device(
    patches,
    embed_weight,
    embed_bias,
    old_in,
    old_out,
    restore_id,
    norm_gains,
    in_biases,
    out_biases,
    final_gain,
    check_weight,
):
    paired = (
        lax.axis_size("col") == 2
        and old_in.shape[0] % 2 == 0
        and (old_in.shape[0] // 2 * old_in.shape[1]) % lax.axis_size("rep") == 0
    )
    if paired:
        in_weight, out_kept, out_arrived = shared_exchange(old_in, old_out)
    else:
        in_weight, out_weight = butterfly_weights(old_in, old_out)
    layer_gain = pick_rows(restore_id, norm_gains)
    in_bias = pick_rows(restore_id, in_biases)
    out_bias = pick_rows(restore_id, out_biases)
    embedded = jnp.dot(patches, embed_weight, preferred_element_type=jnp.float32) + embed_bias
    normed = norm_rows(embedded, layer_gain)
    tokens = lax.all_gather(normed, "col", axis=0, tiled=True)
    chunk_rows = tokens.shape[0] // CHUNKS
    pre_shares = []
    for chunk in range(CHUNKS):
        partial_pre = jnp.dot(
            tokens[chunk * chunk_rows : (chunk + 1) * chunk_rows],
            in_weight,
            preferred_element_type=jnp.float32,
        ).astype(jnp.bfloat16)
        pre_shares.append(
            lax.psum_scatter(partial_pre, "row", scatter_dimension=0, tiled=True)
        )
    hidden_chunks = [
        jax.nn.gelu(share.astype(jnp.float32) + in_bias, approximate=False).astype(jnp.bfloat16)
        for share in pre_shares
    ]
    if paired:
        hidden_chunks[0], out_arrived = lax.optimization_barrier((hidden_chunks[0], out_arrived))
        out_weight = join_out(out_kept, out_arrived)
    partial_branch = jnp.concatenate(
        [
            jnp.dot(
                lax.all_gather(hidden, "row", axis=0, tiled=True),
                out_weight,
                preferred_element_type=jnp.float32,
            ).astype(jnp.bfloat16)
            for hidden in hidden_chunks
        ],
        axis=0,
    )
    updated = (
        embedded
        + lax.psum_scatter(partial_branch, "col", scatter_dimension=0, tiled=True).astype(jnp.float32)
        + out_bias
    )
    final_normed = norm_rows(updated, final_gain)
    check_logits = lax.psum(
        jnp.dot(final_normed, check_weight, preferred_element_type=jnp.float32), "row"
    )
    return (in_weight, out_weight, check_logits)


TAIL_LOG2 = (
    -0.9999999403953552,
    -1.1511064767837524,
    -0.4591980278491974,
    -0.05252550542354584,
    0.0070996368303895,
    -0.00015319570957217366,
    -0.00018990339594893157,
    4.5312575821299106e-05,
    -4.725873623101506e-06,
    1.9546290275229694e-07,
)
TAIL_END = 6.0


def exact_gelu(value):
    size = jnp.abs(value)
    at = jnp.minimum(size, TAIL_END)
    power = TAIL_LOG2[-1]
    for coefficient in TAIL_LOG2[-2::-1]:
        power = power * at + coefficient
    return jnp.maximum(value, 0.0) - size * jnp.exp2(power)


def place_kernel(axis, place_ref, own_ref, early_ref, *refs):
    late_refs, out_ref = refs[:-1], refs[-1]
    col = place_ref[0]
    step = pl.program_id(0)
    rows, cols = own_ref.shape[1:]

    def window(index):
        start = pl.multiple_of(index * (rows, cols)[axis], 128)
        return pl.ds(start, (rows, cols)[axis])

    if axis == 1:
        out_ref[:, window(col)] = own_ref[0]
        out_ref[:, window(1 - col)] = early_ref[0]
        return
    out_ref[window(col)] = own_ref[0]
    out_ref[window(1 - col), : cols // 2] = early_ref[0]
    for number, late_ref in enumerate(late_refs):
        @pl.when(step == number)
        def _(late_ref=late_ref):
            out_ref[window(1 - col), cols // 2 :] = late_ref[...]


def place_tiles(old, arrived, axis, late=()):
    count = arrived.shape[0]
    _, rows, cols = old.shape
    place = jnp.stack([lax.axis_index("col"), lax.axis_index("rep")]).astype(jnp.int32)
    if axis == 0:
        out_shape, out_block = (2 * rows, count * cols), (2 * rows, cols)
        out_map = lambda i, place: (0, place[1] ^ i)
    else:
        out_shape, out_block = (count * rows, 2 * cols), (rows, 2 * cols)
        out_map = lambda i, place: (place[1] ^ i, 0)
    return pl.pallas_call(
        functools.partial(place_kernel, axis),
        grid_spec=pltpu.PrefetchScalarGridSpec(
            num_scalar_prefetch=1,
            grid=(count,),
            in_specs=[
                pl.BlockSpec((1, rows, cols), lambda i, place: (place[0] * count + (place[1] ^ i), 0, 0)),
                pl.BlockSpec((1,) + arrived.shape[1:], lambda i, place: (place[1] ^ i, 0, 0)),
            ]
            + [pl.BlockSpec(piece.shape, lambda i, place: (0, 0)) for piece in late],
            out_specs=pl.BlockSpec(out_block, out_map),
        ),
        out_shape=jax.ShapeDtypeStruct(out_shape, old.dtype),
        compiler_params=pltpu.CompilerParams(vmem_limit_bytes=66_000_000),
        cost_estimate=pl.CostEstimate(
            flops=2 * rows * cols * count * 4096, bytes_accessed=8 * rows * cols * count, transcendentals=0
        ),
        name="place",
    )(place, old, arrived, *late)


MESH = pl.DeviceIdType.MESH
STRIPS = 12
PAIR = 2
ROWS = 4
PASSES = 6
TICK_PASSES = (19,)


def column(row, rows=128):
    return jnp.transpose(jnp.broadcast_to(row, (rows, row.shape[1])))


def gather_kernel(
    patch_size, tok_ref, weight_ref, embed_bias_ref, gain_ref, bias_ref, old_in, old_out,
    embedded_out, in_tiles, in_late, out_tiles, near_kept, near_late, far_got, late_got,
    kept, far_sent, late_sent, sum_kept, sum_late, near, far, lifted, embedded, part, from_outer, from_inner, middle, final, maps, toks, scales, held,
    sums, sums_in, stats, stats_in, scale_sent, scale_in,
    near_sem, tile_sem, embed_sem, sums_sem, stats_sem, scale_sem, far_sem, tok_sem, outer_sem, middle_sem,
    final_sem, keep_sem, across_sem, core_sem, relay_sem, out_sem, out_across_sem, out_core_sem, out_relay_sem,
    kept_sem, got_sem, sum_sem, in_sem,
):
    rep, row, col = lax.axis_index("rep"), lax.axis_index("row"), lax.axis_index("col")
    owners, strips, depth, width = maps.shape
    half_rows = depth // 2
    early = in_tiles.shape[2] // width
    row_count = ROWS
    out_rows = out_tiles.shape[1] // PASSES
    features = weight_ref.shape[1] * row_count
    side = row // 2
    outer = (row == 0) | (row == 3)
    inner = jnp.logical_not(outer)
    own, other = side, 1 - side
    outer_row, inner_row, other_inner = side * 3, 1 + side, 2 - side
    far_col, far_rep, twin = {"col": 1 - col}, {"rep": rep ^ 2}, {"rep": rep ^ 1}
    row_peers = [{"row": (row + step) % row_count} for step in range(1, row_count)]

    barrier = pltpu.get_barrier_semaphore()
    peers = [far_col, far_rep, twin] + row_peers
    for device in peers:
        pl.semaphore_signal(barrier, inc=1, device_id=device, device_id_type=MESH)
    pl.semaphore_wait(barrier, len(peers))

    def remote(source, target, sems, device):
        return pltpu.make_async_remote_copy(
            src_ref=source, dst_ref=target, send_sem=sems.at[0], recv_sem=sems.at[1],
            device_id=device, device_id_type=MESH,
        )

    def columns(strip):
        return pl.ds(pl.multiple_of(strip * width, width), width)

    def half_block(half, strip):
        return maps.at[rep, strip, pl.ds(pl.multiple_of(half * half_rows, 16), half_rows)]

    def fetch_near(strip):
        return pltpu.make_async_copy(
            old_in.at[col * owners + rep, :, columns(strip)], near.at[strip], near_sem.at[strip]
        )

    def fetch_kept(owner):
        return pltpu.make_async_copy(old_out.at[col * owners + owner], kept.at[owner], kept_sem.at[owner])

    def fetch_late(owner):
        return pltpu.make_async_copy(out_tiles.at[owner], kept.at[owner], kept_sem.at[owner])

    def send_sum():
        return remote(far_sent, far_got, got_sem.at[0], far_col)

    def send_late():
        return remote(late_sent, late_got, got_sem.at[1], far_col)

    def keep_sum():
        return pltpu.make_async_copy(sum_kept, near_kept, sum_sem.at[0])

    def keep_late_sum():
        return pltpu.make_async_copy(sum_late, near_late, sum_sem.at[1])

    def send_far(strip):
        source = old_in.at[(1 - col) * owners + rep, :, columns(strip)]
        return remote(source, far.at[strip], far_sem.at[strip], far_col)

    def keep_tile(strip):
        return pltpu.make_async_copy(far.at[strip], in_tiles.at[rep, :, columns(strip)], tile_sem.at[strip])

    def keep_late(strip):
        return pltpu.make_async_copy(far.at[strip], in_late.at[:, columns(strip - early)], tile_sem.at[strip])

    def in_across(strip):
        return remote(far.at[strip], in_tiles.at[rep, :, columns(strip)], in_sem.at[strip, 0], far_rep)

    def in_core(strip):
        return remote(far.at[strip], in_tiles.at[rep, :, columns(strip)], in_sem.at[strip, 1], twin)

    def in_relay(strip):
        block = in_tiles.at[rep ^ 2, :, columns(strip)]
        return remote(block, block, in_sem.at[strip, 2], twin)

    def send_tok():
        return remote(tok_ref, toks.at[1], tok_sem, far_col)

    def send_sums(step):
        return remote(sums, sums_in.at[step], sums_sem.at[step], row_peers[step])

    def send_stats(step):
        return remote(stats, stats_in.at[step], stats_sem.at[step], row_peers[step])

    def send_scale():
        return remote(scale_sent, scale_in, scale_sem, far_col)

    def keep_embedded():
        return pltpu.make_async_copy(embedded, embedded_out, embed_sem)

    def out_block(owner, index):
        return out_tiles.at[owner, pl.ds(index * out_rows, out_rows)]

    def send_out(index):
        source = old_out.at[(1 - col) * owners + rep, pl.ds(index * out_rows, out_rows)]
        return remote(source, out_block(rep, index), out_sem.at[index], far_col)

    def out_across(index):
        return remote(out_block(rep, index), out_block(rep, index), out_across_sem.at[index], far_rep)

    def out_core(index):
        return remote(out_block(rep, index), out_block(rep, index), out_core_sem.at[index], twin)

    def out_relay(index):
        owner = rep ^ 2
        return remote(out_block(owner, index), out_block(owner, index), out_relay_sem.at[index], twin)

    def to_inner(strip, half, slot):
        return remote(part.at[strip, half], from_outer.at[strip, slot], outer_sem.at[strip, slot], {"row": inner_row})

    def to_middle(strip):
        return remote(middle.at[strip], from_inner.at[strip], middle_sem.at[strip], {"row": other_inner})

    def final_across(strip):
        return remote(final.at[strip], half_block(own, strip), final_sem.at[strip, 0], {"row": other_inner})

    def final_arrives(strip):
        return remote(final.at[strip], half_block(other, strip), final_sem.at[strip, 0], {"row": other_inner})

    def final_out(strip):
        return remote(final.at[strip], half_block(own, strip), final_sem.at[strip, 1], {"row": outer_row})

    def final_pass(strip):
        return remote(half_block(other, strip), half_block(other, strip), final_sem.at[strip, 2], {"row": outer_row})

    def final_keep(strip):
        return pltpu.make_async_copy(final.at[strip], half_block(own, strip), keep_sem.at[strip])

    def across(strip):
        return remote(maps.at[rep, strip], maps.at[rep, strip], across_sem.at[strip], far_rep)

    def to_core(strip):
        return remote(maps.at[rep, strip], maps.at[rep, strip], core_sem.at[strip], twin)

    def relay(strip):
        return remote(maps.at[rep ^ 2, strip], maps.at[rep ^ 2, strip], relay_sem.at[strip], twin)

    for strip in range(strips // 2):
        send_far(strip).start()
    for strip in range(strips):
        fetch_near(strip).start()
    for owner in range(owners):
        fetch_kept(owner).start()

    lane = lax.broadcasted_iota(jnp.int32, (8, depth), 1)
    ones = jnp.ones((8, weight_ref.shape[1]), jnp.bfloat16)
    weight_sums = lax.dot_general(
        ones, weight_ref[...], (((1,), (1,)), ((), ())), preferred_element_type=jnp.float32
    )
    sums[...] = jnp.where(lane == patch_size, jnp.sum(embed_bias_ref[...]), weight_sums)
    for step in range(row_count - 1):
        send_sums(step).start()
    toks[0] = tok_ref[...]
    embedded[...] = (
        jnp.dot(tok_ref[...], weight_ref[...], preferred_element_type=jnp.float32) + embed_bias_ref[...]
    )
    values = embedded[...]
    lane = lax.broadcasted_iota(jnp.int32, (values.shape[0], 128), 1)
    total = jnp.sum(values, axis=1, keepdims=True)
    squares = jnp.sum(values * values, axis=1, keepdims=True)
    stats[...] = jnp.transpose(jnp.where(lane == 0, total, squares))[:8]
    for step in range(row_count - 1):
        send_stats(step).start()
    keep_embedded().start()

    for step in range(row_count - 1):
        send_sums(step).wait_recv()
    mean = column((sums[...] + sums_in[0] + sums_in[1] + sums_in[2])[:1] / features)[:, :1]
    extent = lifted.shape[2]
    number = lax.broadcasted_iota(jnp.int32, (depth, extent), 0)
    for half in range(2):
        window = slice(half * extent, (half + 1) * extent)
        raw = jnp.where(
            number == patch_size, embed_bias_ref[:, window], weight_ref[:, window].astype(jnp.float32)
        )
        lifted[half] = ((raw - mean) * gain_ref[:, window]).astype(lifted.dtype)

    for step in range(row_count - 1):
        send_stats(step).wait_recv()
    moments = (stats[...] + stats_in[0] + stats_in[1] + stats_in[2]) / features
    spread = moments[1:2] - moments[:1] * moments[:1]
    scale = lax.rsqrt(spread + EPSILON)
    scale_sent[...] = jnp.broadcast_to(scale, scale_sent.shape)
    send_scale().start()
    for strip in range(strips // 2, strips):
        send_far(strip).start()
    send_tok().start()
    for index in range(PASSES):
        send_out(index).start()
    scales[0] = column(scale)

    def multiply(strip):
        fetch_near(strip).wait()
        send_far(strip).wait_recv()

        @pl.when(strip < early)
        def _():
            keep_tile(strip).start()
            in_across(strip).start()
            in_core(strip).start()

        @pl.when(strip >= early)
        def _():
            keep_late(strip).start()

        total = jnp.dot(lifted[col], near[strip], preferred_element_type=jnp.float32) + jnp.dot(
            lifted[1 - col], far[strip], preferred_element_type=jnp.float32
        )
        part[strip, 0] = total[:half_rows].astype(part.dtype)
        part[strip, 1] = total[half_rows:].astype(part.dtype)

        @pl.when(outer)
        def _():
            to_inner(strip, other, 0).start()
            to_inner(strip, own, 1).start()

    def halfway(strip):
        @pl.when(inner)
        def _():
            to_inner(strip, other, 0).wait_recv()
            middle[strip] = (
                part[strip, other].astype(jnp.float32) + from_outer[strip, 0].astype(jnp.float32)
            ).astype(middle.dtype)
            to_middle(strip).start()

    def finish(strip):
        @pl.when(inner)
        def _():
            to_inner(strip, own, 1).wait_recv()
            to_middle(strip).wait_recv()
            final[strip] = (
                part[strip, own].astype(jnp.float32)
                + from_outer[strip, 1].astype(jnp.float32)
                + from_inner[strip].astype(jnp.float32)
            ).astype(final.dtype)
            final_across(strip).start()
            final_out(strip).start()
            final_keep(strip).start()

    def settle(strip):
        @pl.when(inner)
        def _():
            final_arrives(strip).wait_recv()
            final_pass(strip).start()
            final_keep(strip).wait()
            across(strip).start()
            to_core(strip).start()

    def settle_outer(strip):
        @pl.when(outer)
        def _():
            final_out(strip).wait_recv()
            final_pass(strip).wait_recv()
            across(strip).start()
            to_core(strip).start()

    def hand_on(strip):
        across(strip).wait_recv()
        relay(strip).start()

        @pl.when(strip < early)
        def _():
            in_across(strip).wait_recv()
            in_relay(strip).start()

    block = PAIR * width
    blocks = strips // PAIR

    def owner_of(turn):
        return rep ^ (turn % 2 * 2 + turn // 2)

    def activate(pair, turn, half):
        owner = owner_of(turn)
        unit = (pair * owners + turn) * 2 + half
        applied = jnp.concatenate([maps[owner, pair * PAIR + number] for number in range(PAIR)], axis=1)
        pre = jnp.dot(toks[half], applied, preferred_element_type=jnp.float32)
        scale = jnp.concatenate([scales[half]] * (block // 128), axis=1)
        held[unit] = exact_gelu(pre * scale + bias_ref[owner * blocks + pair]).astype(held.dtype)

    def activate_near(strip):
        @pl.when(strip % PAIR == PAIR - 1)
        def _():
            pair = strip // PAIR

            def piece(turn, carry):
                @pl.when(turn == 2)
                def _():
                    for number in range(PAIR):
                        to_core(pair * PAIR + number).wait_recv()

                @pl.when(turn == 3)
                def _():
                    for number in range(PAIR):
                        relay(pair * PAIR + number).wait_recv()

                activate(pair, turn, 0)
                return carry

            lax.fori_loop(0, owners, piece, 0)

    def pass_out(index):
        if index < PASSES:
            send_out(index).wait_recv()
            out_across(index).start()
            out_core(index).start()
        if index:
            out_across(index - 1).wait_recv()
            out_relay(index - 1).start()

    stages = (
        (0, multiply), (1, halfway), (2, finish), (3, settle), (5, settle_outer), (7, hand_on), (9, activate_near)
    )

    def advance(tick, carry):
        for delay, stage in stages:
            strip = tick - delay

            @pl.when((strip >= 0) & (strip < strips))
            def _(stage=stage, strip=strip):
                stage(strip)

        for index, moment in enumerate(TICK_PASSES):
            @pl.when(tick == moment)
            def _(index=index):
                pass_out(index)

        return carry

    def with_passes(count, first, moments, work):
        def step(number, carry):
            work(number)
            for index, moment in enumerate(moments):
                @pl.when(number == moment)
                def _(index=index):
                    pass_out(first + index)

            return carry

        lax.fori_loop(0, count, step, 0)

    lax.fori_loop(0, strips + stages[-1][0], advance, 0)
    send_tok().wait_recv()
    send_scale().wait_recv()
    scales[1] = column(scale_in[:1])
    pieces = blocks * owners
    with_passes(
        pieces, 1, (pieces // 4, 2 * pieces // 3, pieces - 1),
        lambda number: activate(number // owners, number % owners, 1),
    )
    for owner in range(owners):
        fetch_kept(owner).wait()

    def add_up(half, total):
        def step(turn):
            rows = [held[(pair * owners + turn) * 2 + half] for pair in range(blocks)]
            total[...] += jnp.dot(
                jnp.concatenate(rows, axis=1), kept[owner_of(turn)], preferred_element_type=jnp.float32
            )

        return step

    sum_kept[...] = jnp.zeros_like(sum_kept)
    with_passes(owners, 4, (owners - 1,), add_up(1, sum_kept))
    far_sent[...] = sum_kept[...].astype(far_sent.dtype)
    send_sum().start()
    sum_kept[...] = jnp.zeros_like(sum_kept)
    with_passes(owners, 5, (0,), add_up(0, sum_kept))
    keep_sum().start()

    fetch_late(rep).start()
    pass_out(PASSES)
    for index in range(PASSES):
        out_core(index).wait_recv()
    for turn in (1, 2):
        fetch_late(owner_of(turn)).start()
    for index in range(PASSES):
        out_relay(index).wait_recv()
    fetch_late(owner_of(owners - 1)).start()
    for owner in range(owners):
        fetch_late(owner).wait()
    sum_late[...] = jnp.zeros_like(sum_late)
    with_passes(owners, 0, (), add_up(1, sum_late))
    late_sent[...] = sum_late[...].astype(late_sent.dtype)
    send_late().start()
    sum_late[...] = jnp.zeros_like(sum_late)
    with_passes(owners, 0, (), add_up(0, sum_late))
    keep_late_sum().start()

    def finish_strip(strip, carry):
        for copy in (across(strip), to_core(strip), relay(strip), send_far(strip)):
            copy.wait_send()

        @pl.when(strip < early)
        def _():
            keep_tile(strip).wait()
            in_core(strip).wait()
            in_relay(strip).wait()
            in_across(strip).wait_send()

        @pl.when(strip >= early)
        def _():
            keep_late(strip).wait()

        @pl.when(outer)
        def _():
            to_inner(strip, other, 0).wait_send()
            to_inner(strip, own, 1).wait_send()

        @pl.when(inner)
        def _():
            for copy in (to_middle(strip), final_across(strip), final_out(strip), final_pass(strip)):
                copy.wait_send()

        return carry

    lax.fori_loop(0, strips, finish_strip, 0)

    keep_sum().wait()
    keep_late_sum().wait()
    for step in range(row_count - 1):
        send_sums(step).wait_send()
        send_stats(step).wait_send()
    keep_embedded().wait()
    for copy in (send_scale(), send_tok()):
        copy.wait_send()
    for index in range(PASSES):
        for copy in (send_out(index), out_across(index), out_core(index), out_relay(index)):
            copy.wait_send()
    send_sum().wait()
    send_late().wait()


def gather_hidden(patch_size, tok, weight, embed_bias, gain, in_bias, old_in, old_out):
    rep_count = lax.axis_size("rep")
    tokens, depth = tok.shape
    local = weight.shape[1]
    _, tile_rows, group_cols = old_in.shape
    width, half_rows = group_cols // STRIPS, depth // 2
    any_space = pl.BlockSpec(memory_space=pl.ANY)
    vmem = pl.BlockSpec(memory_space=pltpu.VMEM)
    strip_shape = (half_rows, width)
    units = 2 * rep_count * STRIPS // PAIR
    dma = pltpu.SemaphoreType.DMA
    f32, bf16 = jnp.float32, jnp.bfloat16
    return pl.pallas_call(
        functools.partial(gather_kernel, patch_size),
        out_shape=(
            jax.ShapeDtypeStruct((tokens, local), f32),
            jax.ShapeDtypeStruct((rep_count, tile_rows, group_cols // 2), old_in.dtype),
            jax.ShapeDtypeStruct((tile_rows, group_cols // 2), old_in.dtype),
            jax.ShapeDtypeStruct((rep_count,) + old_out.shape[1:], old_out.dtype),
            jax.ShapeDtypeStruct((tokens, tile_rows), f32),
            jax.ShapeDtypeStruct((tokens, tile_rows), f32),
            jax.ShapeDtypeStruct((tokens, tile_rows), bf16),
            jax.ShapeDtypeStruct((tokens, tile_rows), bf16),
        ),
        in_specs=[vmem] * 5 + [any_space] * 2,
        out_specs=(any_space,) * 8,
        scratch_shapes=[
            pltpu.VMEM((rep_count,) + old_out.shape[1:], old_out.dtype),
            pltpu.VMEM((tokens, tile_rows), bf16),
            pltpu.VMEM((tokens, tile_rows), bf16),
            pltpu.VMEM((tokens, tile_rows), f32),
            pltpu.VMEM((tokens, tile_rows), f32),
            pltpu.VMEM((STRIPS, tile_rows, width), old_in.dtype),
            pltpu.VMEM((STRIPS, tile_rows, width), old_in.dtype),
            pltpu.VMEM((2, depth, tile_rows), bf16),
            pltpu.VMEM((tokens, local), f32),
            pltpu.VMEM((STRIPS, 2) + strip_shape, bf16),
            pltpu.VMEM((STRIPS, 2) + strip_shape, bf16),
            pltpu.VMEM((STRIPS,) + strip_shape, bf16),
            pltpu.VMEM((STRIPS,) + strip_shape, bf16),
            pltpu.VMEM((STRIPS,) + strip_shape, bf16),
            pltpu.VMEM((rep_count, STRIPS, depth, width), bf16),
            pltpu.VMEM((2, tokens, depth), bf16),
            pltpu.VMEM((2, tokens, 128), f32),
            pltpu.VMEM((units, tokens, PAIR * width), bf16),
            pltpu.VMEM((8, depth), f32),
            pltpu.VMEM((ROWS - 1, 8, depth), f32),
            pltpu.VMEM((8, tokens), f32),
            pltpu.VMEM((ROWS - 1, 8, tokens), f32),
            pltpu.VMEM((8, tokens), f32),
            pltpu.VMEM((8, tokens), f32),
            dma((STRIPS,)),
            dma((STRIPS,)),
            dma,
            dma((ROWS - 1, 2)),
            dma((ROWS - 1, 2)),
            dma((2,)),
            dma((STRIPS, 2)),
            dma((2,)),
            dma((STRIPS, 2, 2)),
            dma((STRIPS, 2)),
            dma((STRIPS, 3, 2)),
            dma((STRIPS,)),
            dma((STRIPS, 2)),
            dma((STRIPS, 2)),
            dma((STRIPS, 2)),
            dma((PASSES, 2)),
            dma((PASSES, 2)),
            dma((PASSES, 2)),
            dma((PASSES, 2)),
            dma((rep_count,)),
            dma((2, 2)),
            dma((2,)),
            dma((STRIPS // 2, 3, 2)),
        ],
        compiler_params=pltpu.CompilerParams(
            collective_id=0, has_side_effects=True, vmem_limit_bytes=66_000_000
        ),
        cost_estimate=pl.CostEstimate(flops=10**10, bytes_accessed=10**8, transcendentals=0),
        name="gather_hidden",
    )(tok, weight, embed_bias[None], gain[None], in_bias.reshape(-1, 1, PAIR * width), old_in, old_out)


def rep_partner(value, mask):
    return lax.ppermute(value, "rep", [(s, s ^ mask) for s in range(lax.axis_size("rep"))])


def after(value, *others):
    return lax.optimization_barrier((value,) + others)[0]


def row_of(restore_id, table):
    return lax.dynamic_slice_in_dim(table, restore_id[0], 1, axis=0)[0]


def fast_device(
    patches,
    embed_weight,
    embed_bias,
    old_in,
    old_out,
    restore_id,
    norm_gains,
    in_biases,
    out_biases,
    final_gain,
    check_weight,
):
    col = lax.axis_index("col")
    row_count = lax.axis_size("row")
    token_count, patch_size = patches.shape
    feature_count = embed_weight.shape[1] * row_count
    depth = -(-(patch_size + 1) // 32) * 32

    layer_gain = row_of(restore_id, norm_gains)
    in_bias = row_of(restore_id, in_biases)
    out_bias = row_of(restore_id, out_biases)

    check32 = check_weight.astype(jnp.float32) * final_gain[:, None]
    tok = jnp.concatenate(
        (
            patches,
            jnp.ones((token_count, 1), patches.dtype),
            jnp.zeros((token_count, depth - patch_size - 1), patches.dtype),
        ),
        axis=1,
    )
    weight = jnp.pad(embed_weight, ((0, depth - patch_size), (0, 0)))
    embedded, in_tiles, in_late, out_tiles, near_kept, near_late, far_got, late_got = gather_hidden(
        patch_size, tok, weight, embed_bias, layer_gain, in_bias, old_in, old_out
    )
    late_across = rep_partner(in_late, 2)
    late_core = rep_partner(in_late, 1)
    branch_parts = (
        near_kept + late_got.astype(jnp.float32),
        near_late + far_got.astype(jnp.float32),
    )
    branch = jnp.where(
        col == 0, jnp.concatenate(branch_parts, axis=1), jnp.concatenate(branch_parts[::-1], axis=1)
    )
    updated = embedded + branch + out_bias

    def halves(value):
        upper = lax.reduce_precision(value, 8, 7)
        return upper.astype(jnp.bfloat16), (value - upper).astype(jnp.bfloat16)

    updated_hi, updated_lo = halves(updated)
    check_hi, check_lo = halves(check32)
    raw = (
        jnp.dot(updated_hi, check_hi, preferred_element_type=jnp.float32)
        + jnp.dot(updated_lo, check_hi, preferred_element_type=jnp.float32)
        + jnp.dot(updated_hi, check_lo, preferred_element_type=jnp.float32)
    )
    shares = (raw, jnp.sum(updated, axis=1), jnp.sum(updated * updated, axis=1))
    out_tiles = after(out_tiles, *shares)
    raw = lax.psum(shares[0], "row")
    total, squares = lax.psum(shares[1:], "row")
    check_sum = lax.psum(jnp.sum(check32, axis=0), "row")
    out_weight = place_tiles(old_out, out_tiles, 1)
    late_relay = rep_partner(after(late_across, out_weight), 1)
    in_weight = place_tiles(old_in, in_tiles, 0, (in_late, late_core, late_across, late_relay))
    raw, in_weight, out_weight = lax.optimization_barrier((raw, in_weight, out_weight))
    average = (total / feature_count)[:, None]
    spread = (squares / feature_count)[:, None] - average * average
    check_logits = lax.rsqrt(spread + EPSILON) * (raw - average * check_sum)
    return (in_weight, out_weight, check_logits)


def on_either(*args):
    old_in = args[3]
    shared = (
        lax.axis_size("col") == 2
        and lax.axis_size("rep") == 4
        and lax.axis_size("row") == ROWS
        and old_in.shape[0] == 2 * lax.axis_size("rep")
    )
    return fast_device(*args) if shared else on_device(*args)


def solution(mesh):
    placed = (
        P(("rep", "col"), None),
        P(None, "row"),
        P("row"),
        P(("row", "col"), None, None),
        P(("row", "col"), None, None),
        P(),
        P(None, "row"),
        P(None, "col"),
        P(None, "row"),
        P("row"),
        P("row", None),
    )
    return jax.shard_map(
        on_either,
        mesh=mesh,
        in_specs=placed,
        out_specs=(P("row", "col"), P("col", "row"), P(("rep", "col"), None)),
        check_vma=False,
    )
```

```python
import functools

import jax
import jax.numpy as jnp
from jax import lax
from jax.experimental import pallas as pl
from jax.experimental.pallas import tpu as pltpu
from jax.sharding import PartitionSpec as P

EPSILON = 1e-06
CHUNKS = 2


def for_sending(shard):
    return jax.tree.map(lambda a: a.astype(jnp.bfloat16) if a.dtype == jnp.float32 else a, shard)


def partner(value, axis, bit):
    mask = 2**bit
    pairs = [(source, source ^ mask) for source in range(lax.axis_size(axis))]
    return lax.ppermute(value, axis, pairs)


def pick_rows(restore_id, param_table):
    selector = (
        jnp.arange(param_table.shape[0], dtype=jnp.int32)[None, :] == restore_id[:, None]
    ).astype(jnp.float32)
    return jnp.dot(selector, param_table, precision=lax.Precision.HIGHEST)[0]


def norm_rows(values, gain_row):
    feature_count = values.shape[1] * lax.axis_size("row")
    totals = lax.psum((jnp.sum(values, axis=1), jnp.sum(values * values, axis=1)), "row")
    average = totals[0][:, None] / feature_count
    spread = totals[1][:, None] / feature_count - average * average
    return ((values - average) * lax.rsqrt(spread + EPSILON) * gain_row).astype(jnp.bfloat16)


def move_halves(pieces, bit_total, device_index, exchange):
    for bit_number in range(bit_total):
        upper_side = device_index >> bit_number & 1 == 1
        outgoing = tuple(
            (jnp.where(upper_side, lower_part, upper_part) for lower_part, upper_part in pieces)
        )
        incoming = exchange(outgoing, bit_number)
        pieces = tuple(
            (
                (
                    jnp.where(upper_side, arrived, lower_part),
                    jnp.where(upper_side, upper_part, arrived),
                )
                for (lower_part, upper_part), arrived in zip(pieces, incoming)
            )
        )
    return pieces


def butterfly_weights(old_in, old_out):
    tiles_here, tile_rows, tile_cols = old_in.shape
    local_cols = tiles_here * tile_cols
    half_cols = local_cols // 2
    in_local = jnp.transpose(old_in, (1, 0, 2)).reshape(tile_rows, local_cols)
    out_local = old_out.reshape(local_cols, tile_rows)
    col_index = lax.axis_index("col")
    col_count = lax.axis_size("col")
    col_bits = col_count.bit_length() - 1
    pieces = (
        (in_local[:, :half_cols], in_local[:, half_cols:]),
        (out_local[:half_cols], out_local[half_cols:]),
    )
    pieces = move_halves(
        pieces,
        col_bits,
        col_index,
        lambda send_parts, bit_number: jax.tree.map(
            lambda part, own: part.astype(own.dtype),
            partner(for_sending(send_parts), "col", bit_number),
            send_parts,
        ),
    )
    in_pair, out_pair = pieces
    in_weight = jnp.concatenate(in_pair, axis=0)
    out_weight = jnp.concatenate(out_pair, axis=1)
    return in_weight, out_weight


def shared_exchange(old_in, old_out):
    tiles_here, tile_rows, tile_cols = old_in.shape
    half_tiles = tiles_here // 2
    half_cols = half_tiles * tile_cols
    col_index = lax.axis_index("col")
    rep_index = lax.axis_index("rep")
    rep_count = lax.axis_size("rep")
    in_parts = old_in.reshape(2, rep_count, half_tiles * tile_rows // rep_count, tile_cols)
    share = lax.dynamic_slice(
        in_parts, (1 - col_index, rep_index, 0, 0), (1, 1) + in_parts.shape[2:]
    )[0, 0]
    share = partner(share, "col", 0)
    out_parts = old_out.reshape(2, half_cols, tile_rows)
    out_sent = lax.dynamic_index_in_dim(out_parts, 1 - col_index, 0, keepdims=False)
    out_kept = lax.dynamic_index_in_dim(out_parts, col_index, 0, keepdims=False)
    share, out_sent = lax.optimization_barrier((share, out_sent))
    out_arrived = partner(out_sent, "col", 0)
    in_arrived = lax.all_gather(share, "rep", axis=0, tiled=True)

    def as_rows(tiles):
        rows = tiles.reshape(half_tiles, tile_rows, tile_cols)
        return jnp.transpose(rows, (1, 0, 2)).reshape(1, tile_rows, half_cols)

    kept = as_rows(lax.dynamic_index_in_dim(in_parts, col_index, 0, keepdims=False))
    blocks = jnp.zeros((2, tile_rows, half_cols), old_in.dtype)
    blocks = lax.dynamic_update_slice(blocks, kept, (col_index, 0, 0))
    blocks = lax.dynamic_update_slice(blocks, as_rows(in_arrived), (1 - col_index, 0, 0))
    return blocks.reshape(2 * tile_rows, half_cols), out_kept, out_arrived


def join_out(out_kept, out_arrived):
    upper_side = lax.axis_index("col") == 1
    return jnp.concatenate(
        (
            jnp.where(upper_side, out_arrived, out_kept),
            jnp.where(upper_side, out_kept, out_arrived),
        ),
        axis=1,
    )


def on_device(
    patches,
    embed_weight,
    embed_bias,
    old_in,
    old_out,
    restore_id,
    norm_gains,
    in_biases,
    out_biases,
    final_gain,
    check_weight,
):
    paired = (
        lax.axis_size("col") == 2
        and old_in.shape[0] % 2 == 0
        and (old_in.shape[0] // 2 * old_in.shape[1]) % lax.axis_size("rep") == 0
    )
    if paired:
        in_weight, out_kept, out_arrived = shared_exchange(old_in, old_out)
    else:
        in_weight, out_weight = butterfly_weights(old_in, old_out)
    layer_gain = pick_rows(restore_id, norm_gains)
    in_bias = pick_rows(restore_id, in_biases)
    out_bias = pick_rows(restore_id, out_biases)
    embedded = jnp.dot(patches, embed_weight, preferred_element_type=jnp.float32) + embed_bias
    normed = norm_rows(embedded, layer_gain)
    tokens = lax.all_gather(normed, "col", axis=0, tiled=True)
    chunk_rows = tokens.shape[0] // CHUNKS
    pre_shares = []
    for chunk in range(CHUNKS):
        partial_pre = jnp.dot(
            tokens[chunk * chunk_rows : (chunk + 1) * chunk_rows],
            in_weight,
            preferred_element_type=jnp.float32,
        ).astype(jnp.bfloat16)
        pre_shares.append(
            lax.psum_scatter(partial_pre, "row", scatter_dimension=0, tiled=True)
        )
    hidden_chunks = [
        jax.nn.gelu(share.astype(jnp.float32) + in_bias, approximate=False).astype(jnp.bfloat16)
        for share in pre_shares
    ]
    if paired:
        hidden_chunks[0], out_arrived = lax.optimization_barrier((hidden_chunks[0], out_arrived))
        out_weight = join_out(out_kept, out_arrived)
    partial_branch = jnp.concatenate(
        [
            jnp.dot(
                lax.all_gather(hidden, "row", axis=0, tiled=True),
                out_weight,
                preferred_element_type=jnp.float32,
            ).astype(jnp.bfloat16)
            for hidden in hidden_chunks
        ],
        axis=0,
    )
    updated = (
        embedded
        + lax.psum_scatter(partial_branch, "col", scatter_dimension=0, tiled=True).astype(jnp.float32)
        + out_bias
    )
    final_normed = norm_rows(updated, final_gain)
    check_logits = lax.psum(
        jnp.dot(final_normed, check_weight, preferred_element_type=jnp.float32), "row"
    )
    return (in_weight, out_weight, check_logits)

TAIL_LOG2 = (
    -0.9999999403953552,
    -1.1511064767837524,
    -0.4591980278491974,
    -0.05252550542354584,
    0.0070996368303895,
    -0.00015319570957217366,
    -0.00018990339594893157,
    4.5312575821299106e-05,
    -4.725873623101506e-06,
    1.9546290275229694e-07,
)
TAIL_END = 6.0


def exact_gelu(value):
    size = jnp.abs(value)
    at = jnp.minimum(size, TAIL_END)
    power = TAIL_LOG2[-1]
    for coefficient in TAIL_LOG2[-2::-1]:
        power = power * at + coefficient
    return jnp.maximum(value, 0.0) - size * jnp.exp2(power)


def place_kernel(axis, place_ref, own_ref, arrived_ref, out_ref):
    col = place_ref[0]
    extent = own_ref.shape[1 + axis]
    for index, tile_ref in ((col, own_ref), (1 - col, arrived_ref)):
        window = pl.ds(pl.multiple_of(index * extent, 128), extent)
        if axis == 0:
            out_ref[window] = tile_ref[0]
        else:
            out_ref[:, window] = tile_ref[0]


def place_tiles(old, arrived, axis):
    count = arrived.shape[0]
    _, rows, cols = old.shape
    place = lax.axis_index("col").astype(jnp.int32)[None]
    if axis == 0:
        out_shape, out_block = (2 * rows, count * cols), (2 * rows, cols)
        out_map = lambda i, place: (0, i)
    else:
        out_shape, out_block = (count * rows, 2 * cols), (rows, 2 * cols)
        out_map = lambda i, place: (i, 0)
    return pl.pallas_call(
        functools.partial(place_kernel, axis),
        grid_spec=pltpu.PrefetchScalarGridSpec(
            num_scalar_prefetch=1,
            grid=(count,),
            in_specs=[
                pl.BlockSpec((1, rows, cols), lambda i, place: (place[0] * count + i, 0, 0)),
                pl.BlockSpec((1,) + arrived.shape[1:], lambda i, place: (i, 0, 0)),
            ],
            out_specs=pl.BlockSpec(out_block, out_map),
        ),
        out_shape=jax.ShapeDtypeStruct(out_shape, old.dtype),
        compiler_params=pltpu.CompilerParams(vmem_limit_bytes=66_000_000),
        cost_estimate=pl.CostEstimate(
            flops=2 * rows * cols * count * 4096, bytes_accessed=8 * rows * cols * count, transcendentals=0
        ),
        name="place",
    )(place, old, arrived)


MESH = pl.DeviceIdType.MESH
STRIPS = 12
PAIR = 2
ROWS = 4
PASSES = 12
LAG = 2
TICK_PASSES = (18, 19, 20)


def column(row, rows=128):
    return jnp.transpose(jnp.broadcast_to(row, (rows, row.shape[1])))


def gather_kernel(
    patch_size, tok_ref, weight_ref, rows_ref, check_ref, bias_ref, old_in, old_out,
    in_tiles, out_tiles, logits_ref,
    shares, side_check, shares_sent, shares_in, ends, ends_in, check_hi, check_lo, far_got, late_got, kept, far_sent, late_sent, sum_kept, sum_late, near, far, lifted, embedded, part, from_outer, from_inner, middle, final, maps, toks, scales, held,
    sums, sums_in, stats, stats_in, scale_sent, scale_in,
    near_sem, tile_sem, sums_sem, stats_sem, scale_sem, far_sem, tok_sem, outer_sem, middle_sem,
    final_sem, keep_sem, across_sem, core_sem, relay_sem, out_sem, out_across_sem, out_core_sem, out_relay_sem,
    kept_sem, got_sem, in_sem, shares_sem, ends_sem,
):
    rep, row, col = lax.axis_index("rep"), lax.axis_index("row"), lax.axis_index("col")
    owners, strips, depth, width = maps.shape
    half_rows = depth // 2
    early = strips // 2
    row_count = ROWS
    out_rows = out_tiles.shape[1] // PASSES
    features = weight_ref.shape[1] * row_count
    side = row // 2
    outer = (row == 0) | (row == 3)
    inner = jnp.logical_not(outer)
    own, other = side, 1 - side
    outer_row, inner_row, other_inner = side * 3, 1 + side, 2 - side
    far_col, far_rep, twin = {"col": 1 - col}, {"rep": rep ^ 2}, {"rep": rep ^ 1}
    row_peers = [{"row": (row + step) % row_count} for step in range(1, row_count)]

    barrier = pltpu.get_barrier_semaphore()
    peers = [far_col, far_rep, twin] + row_peers
    for device in peers:
        pl.semaphore_signal(barrier, inc=1, device_id=device, device_id_type=MESH)
    pl.semaphore_wait(barrier, len(peers))

    def remote(source, target, sems, device):
        return pltpu.make_async_remote_copy(
            src_ref=source, dst_ref=target, send_sem=sems.at[0], recv_sem=sems.at[1],
            device_id=device, device_id_type=MESH,
        )

    def columns(strip):
        return pl.ds(pl.multiple_of(strip * width, width), width)

    def half_block(half, strip):
        return maps.at[rep, strip, pl.ds(pl.multiple_of(half * half_rows, 16), half_rows)]

    def fetch_near(strip):
        return pltpu.make_async_copy(
            old_in.at[col * owners + rep, :, columns(strip)], near.at[strip], near_sem.at[strip]
        )

    def fetch_kept(owner):
        return pltpu.make_async_copy(old_out.at[col * owners + owner], kept.at[owner], kept_sem.at[owner])

    def fetch_late(owner):
        return pltpu.make_async_copy(out_tiles.at[owner], kept.at[owner], kept_sem.at[owner])

    def send_sum():
        return remote(far_sent, far_got, got_sem.at[0], far_col)

    def send_late():
        return remote(late_sent, late_got, got_sem.at[1], far_col)

    def send_far(strip):
        source = old_in.at[(1 - col) * owners + rep, :, columns(strip)]
        return remote(source, far.at[strip], far_sem.at[strip], far_col)

    def keep_tile(strip):
        return pltpu.make_async_copy(far.at[strip], in_tiles.at[rep, :, columns(strip)], tile_sem.at[strip])

    def in_across(strip):
        return remote(far.at[strip], in_tiles.at[rep, :, columns(strip)], in_sem.at[strip, 0], far_rep)

    def in_core(strip):
        return remote(far.at[strip], in_tiles.at[rep, :, columns(strip)], in_sem.at[strip, 1], twin)

    def in_relay(strip):
        block = in_tiles.at[rep ^ 2, :, columns(strip)]
        return remote(block, block, in_sem.at[strip, 2], twin)

    def send_tok():
        return remote(tok_ref, toks.at[1], tok_sem, far_col)

    def send_sums(step):
        return remote(sums, sums_in.at[step], sums_sem.at[step], row_peers[step])

    def send_stats(step):
        return remote(stats, stats_in.at[step], stats_sem.at[step], row_peers[step])

    def send_shares(step):
        return remote(shares_sent, shares_in.at[step], shares_sem.at[step], row_peers[step])

    def send_ends(step):
        return remote(ends, ends_in.at[step], ends_sem.at[step], row_peers[step])

    def send_scale():
        return remote(scale_sent, scale_in, scale_sem, far_col)

    def out_block(owner, index):
        return out_tiles.at[owner, pl.ds(index * out_rows, out_rows)]

    def send_out(index):
        source = old_out.at[(1 - col) * owners + rep, pl.ds(index * out_rows, out_rows)]
        return remote(source, out_block(rep, index), out_sem.at[index], far_col)

    def out_across(index):
        return remote(out_block(rep, index), out_block(rep, index), out_across_sem.at[index], far_rep)

    def out_core(index):
        return remote(out_block(rep, index), out_block(rep, index), out_core_sem.at[index], twin)

    def out_relay(index):
        owner = rep ^ 2
        return remote(out_block(owner, index), out_block(owner, index), out_relay_sem.at[index], twin)

    def to_inner(strip, half, slot):
        return remote(part.at[strip, half], from_outer.at[strip, slot], outer_sem.at[strip, slot], {"row": inner_row})

    def to_middle(strip):
        return remote(middle.at[strip], from_inner.at[strip], middle_sem.at[strip], {"row": other_inner})

    def final_across(strip):
        return remote(final.at[strip], half_block(own, strip), final_sem.at[strip, 0], {"row": other_inner})

    def final_arrives(strip):
        return remote(final.at[strip], half_block(other, strip), final_sem.at[strip, 0], {"row": other_inner})

    def final_out(strip):
        return remote(final.at[strip], half_block(own, strip), final_sem.at[strip, 1], {"row": outer_row})

    def final_pass(strip):
        return remote(half_block(other, strip), half_block(other, strip), final_sem.at[strip, 2], {"row": outer_row})

    def final_keep(strip):
        return pltpu.make_async_copy(final.at[strip], half_block(own, strip), keep_sem.at[strip])

    def across(strip):
        return remote(maps.at[rep, strip], maps.at[rep, strip], across_sem.at[strip], far_rep)

    def to_core(strip):
        return remote(maps.at[rep, strip], maps.at[rep, strip], core_sem.at[strip], twin)

    def relay(strip):
        return remote(maps.at[rep ^ 2, strip], maps.at[rep ^ 2, strip], relay_sem.at[strip], twin)

    for strip in range(strips // 2):
        send_far(strip).start()
    for strip in range(strips):
        fetch_near(strip).start()
    for owner in range(owners):
        fetch_kept(owner).start()

    lane = lax.broadcasted_iota(jnp.int32, (8, depth), 1)
    ones = jnp.ones((8, weight_ref.shape[1]), jnp.bfloat16)
    weight_sums = lax.dot_general(
        ones, weight_ref[...], (((1,), (1,)), ((), ())), preferred_element_type=jnp.float32
    )
    sums[...] = jnp.where(lane == patch_size, jnp.sum(rows_ref[:1]), weight_sums)
    for step in range(row_count - 1):
        send_sums(step).start()
    toks[0] = tok_ref[...]
    embedded[...] = (
        jnp.dot(tok_ref[...], weight_ref[...], preferred_element_type=jnp.float32) + rows_ref[:1]
    )
    values = embedded[...]
    lane = lax.broadcasted_iota(jnp.int32, (values.shape[0], 128), 1)
    total = jnp.sum(values, axis=1, keepdims=True)
    squares = jnp.sum(values * values, axis=1, keepdims=True)
    stats[...] = jnp.transpose(jnp.where(lane == 0, total, squares))[:8]
    for step in range(row_count - 1):
        send_stats(step).start()

    check = check_ref[...].astype(jnp.float32) * column(rows_ref[2:3])
    check_hi[...] = check.astype(check_hi.dtype)
    check_lo[...] = (check - check_hi[...].astype(jnp.float32)).astype(check_lo.dtype)
    side_check[...] = jnp.broadcast_to(jnp.sum(check, axis=0, keepdims=True), side_check.shape)
    for step in range(row_count - 1):
        send_sums(step).wait_recv()
    mean = column((sums[...] + sums_in[0] + sums_in[1] + sums_in[2])[:1] / features)[:, :1]
    extent = lifted.shape[2]
    number = lax.broadcasted_iota(jnp.int32, (depth, extent), 0)
    for half in range(2):
        window = slice(half * extent, (half + 1) * extent)
        raw = jnp.where(
            number == patch_size, rows_ref[:1, window], weight_ref[:, window].astype(jnp.float32)
        )
        lifted[half] = ((raw - mean) * rows_ref[1:2, window]).astype(lifted.dtype)

    for step in range(row_count - 1):
        send_stats(step).wait_recv()
    moments = (stats[...] + stats_in[0] + stats_in[1] + stats_in[2]) / features
    spread = moments[1:2] - moments[:1] * moments[:1]
    scale = lax.rsqrt(spread + EPSILON)
    scale_sent[...] = jnp.broadcast_to(scale, scale_sent.shape)
    send_scale().start()
    for strip in range(strips // 2, strips):
        send_far(strip).start()
    send_tok().start()
    for index in range(PASSES):
        send_out(index).start()
    scales[0] = column(scale)

    def multiply(strip):
        fetch_near(strip).wait()
        send_far(strip).wait_recv()

        keep_tile(strip).start()
        in_core(strip).start()

        @pl.when(strip < early)
        def _():
            in_across(strip).start()

        total = jnp.dot(lifted[col], near[strip], preferred_element_type=jnp.float32) + jnp.dot(
            lifted[1 - col], far[strip], preferred_element_type=jnp.float32
        )
        part[strip, 0] = total[:half_rows].astype(part.dtype)
        part[strip, 1] = total[half_rows:].astype(part.dtype)

        @pl.when(outer)
        def _():
            to_inner(strip, other, 0).start()
            to_inner(strip, own, 1).start()

    def halfway(strip):
        @pl.when(inner)
        def _():
            to_inner(strip, other, 0).wait_recv()
            middle[strip] = (
                part[strip, other].astype(jnp.float32) + from_outer[strip, 0].astype(jnp.float32)
            ).astype(middle.dtype)
            to_middle(strip).start()

    def finish(strip):
        @pl.when(inner)
        def _():
            to_inner(strip, own, 1).wait_recv()
            to_middle(strip).wait_recv()
            final[strip] = (
                part[strip, own].astype(jnp.float32)
                + from_outer[strip, 1].astype(jnp.float32)
                + from_inner[strip].astype(jnp.float32)
            ).astype(final.dtype)
            final_across(strip).start()
            final_out(strip).start()
            final_keep(strip).start()

    def settle(strip):
        @pl.when(inner)
        def _():
            final_arrives(strip).wait_recv()
            final_pass(strip).start()
            final_keep(strip).wait()
            across(strip).start()
            to_core(strip).start()

    def settle_outer(strip):
        @pl.when(outer)
        def _():
            final_out(strip).wait_recv()
            final_pass(strip).wait_recv()
            across(strip).start()
            to_core(strip).start()

    def hand_on(strip):
        across(strip).wait_recv()
        relay(strip).start()

        @pl.when(strip < early)
        def _():
            in_across(strip).wait_recv()
            in_relay(strip).start()

    block = PAIR * width
    blocks = strips // PAIR

    def owner_of(turn):
        return rep ^ (turn % 2 * 2 + turn // 2)

    def activate(pair, turn, half):
        owner = owner_of(turn)
        unit = (pair * owners + turn) * 2 + half
        applied = jnp.concatenate([maps[owner, pair * PAIR + number] for number in range(PAIR)], axis=1)
        pre = jnp.dot(toks[half], applied, preferred_element_type=jnp.float32)
        scale = jnp.concatenate([scales[half]] * (block // 128), axis=1)
        held[unit] = exact_gelu(pre * scale + bias_ref[owner * blocks + pair]).astype(held.dtype)

    def activate_near(strip):
        @pl.when(strip % PAIR == PAIR - 1)
        def _():
            pair = strip // PAIR

            def piece(turn, carry):
                @pl.when(turn == 2)
                def _():
                    for number in range(PAIR):
                        to_core(pair * PAIR + number).wait_recv()

                @pl.when(turn == 3)
                def _():
                    for number in range(PAIR):
                        relay(pair * PAIR + number).wait_recv()

                activate(pair, turn, 0)
                return carry

            lax.fori_loop(0, owners, piece, 0)

    def pass_out(index):
        if index < PASSES:
            send_out(index).wait_recv()
            out_across(index).start()
            out_core(index).start()
        if index >= LAG:
            out_across(index - LAG).wait_recv()
            out_relay(index - LAG).start()

    stages = (
        (0, multiply), (1, halfway), (2, finish), (3, settle), (5, settle_outer), (7, hand_on), (9, activate_near)
    )

    def advance(tick, carry):
        for delay, stage in stages:
            strip = tick - delay

            @pl.when((strip >= 0) & (strip < strips))
            def _(stage=stage, strip=strip):
                stage(strip)

        for index, moment in enumerate(TICK_PASSES):
            @pl.when(tick == moment)
            def _(index=index):
                pass_out(index)

        return carry

    def with_passes(count, first, moments, work):
        def step(number, carry):
            work(number)
            for index, moment in enumerate(moments):
                @pl.when(number == moment)
                def _(index=index):
                    pass_out(first + index)

            return carry

        lax.fori_loop(0, count, step, 0)

    lax.fori_loop(0, strips + stages[-1][0], advance, 0)
    send_tok().wait_recv()
    send_scale().wait_recv()
    scales[1] = column(scale_in[:1])
    pieces = blocks * owners
    with_passes(
        pieces, 3, (2, 6, 10, 14, 18, 22),
        lambda number: activate(number // owners, number % owners, 1),
    )
    for owner in range(owners):
        fetch_kept(owner).wait()

    def add_up(half, total):
        def step(turn):
            rows = [held[(pair * owners + turn) * 2 + half] for pair in range(blocks)]
            total[...] += jnp.dot(
                jnp.concatenate(rows, axis=1), kept[owner_of(turn)], preferred_element_type=jnp.float32
            )

        return step

    for step in range(row_count - 1):
        send_sums(step).wait_send()
        send_stats(step).wait_send()
    sum_kept[...] = jnp.zeros_like(sum_kept)
    with_passes(owners, 9, (0, owners - 1), add_up(1, sum_kept))
    far_sent[...] = sum_kept[...].astype(far_sent.dtype)
    send_sum().start()
    sum_kept[...] = jnp.zeros_like(sum_kept)
    with_passes(owners, 11, (0,), add_up(0, sum_kept))

    fetch_late(rep).start()
    for strip in range(strips // 2, strips):
        in_across(strip).start()
    for index in range(PASSES):
        out_core(index).wait_recv()
    fetch_late(owner_of(2)).start()
    for index in range(PASSES, PASSES + LAG):
        pass_out(index)
    fetch_late(owner_of(1)).start()
    sum_late[...] = jnp.zeros_like(sum_late)

    def add_late(number, carry):
        turn = number % 2 * 2 + number // 2
        fetch_late(owner_of(turn)).wait()

        @pl.when(number == 1)
        def _():
            for index in range(PASSES):
                out_relay(index).wait_recv()
            fetch_late(owner_of(owners - 1)).start()

        add_up(1, sum_late)(turn)
        return carry

    lax.fori_loop(0, owners, add_late, 0)
    late_sent[...] = sum_late[...].astype(late_sent.dtype)
    send_late().start()
    sum_late[...] = jnp.zeros_like(sum_late)
    with_passes(owners, 0, (), add_up(0, sum_late))

    def update(half, total, got):
        window = pl.ds(pl.multiple_of(half * extent, extent), extent)
        updated = embedded[:, window] + total[...] + got[...].astype(jnp.float32) + rows_ref[3:4, window]
        upper = updated.astype(jnp.bfloat16)
        lower = (updated - upper.astype(jnp.float32)).astype(jnp.bfloat16)
        logits = (
            jnp.dot(upper, check_hi[window], preferred_element_type=jnp.float32)
            + jnp.dot(lower, check_hi[window], preferred_element_type=jnp.float32)
            + jnp.dot(upper, check_lo[window], preferred_element_type=jnp.float32)
        )
        total = jnp.sum(updated, axis=1, keepdims=True)
        squares = jnp.sum(updated * updated, axis=1, keepdims=True)
        return logits, jnp.where(lane == 0, total, squares)

    send_sum().wait_recv()
    logits, sides = update(1 - col, sum_late, far_got)
    shares[...] = logits
    stats[...] = jnp.transpose(sides)[:8]
    send_late().wait_recv()
    logits, sides = update(col, sum_kept, late_got)
    shares[...] += logits
    local = weight_ref.shape[1]
    ends[...] = stats[...] + jnp.transpose(sides)[:8]
    ends[2:3, :128] = side_check[:1]
    centered = shares[...] - column(ends[:1] / local) * side_check[:1]
    shares_sent[...] = centered.astype(shares_sent.dtype)
    for step in range(row_count - 1):
        send_ends(step).start()
        send_shares(step).start()
    for step in range(row_count - 1):
        send_ends(step).wait_recv()
    every = [ends[...]] + [ends_in[step] for step in range(row_count - 1)]
    moments = sum(every[1:], every[0]) / features
    mean = moments[:1]
    scale = column(lax.rsqrt(moments[1:2] - mean * mean + EPSILON))
    for side in every:
        centered = centered + column(side[:1] / local - mean) * side[2:3, :128]
    for step in range(row_count - 1):
        send_shares(step).wait_recv()
        centered = centered + shares_in[step].astype(jnp.float32)
    logits_ref[...] = scale * centered
    for step in range(row_count - 1):
        send_ends(step).wait_send()
        send_shares(step).wait_send()
    for strip in range(strips // 2, strips):
        in_across(strip).wait_recv()
        in_relay(strip).start()

    def finish_strip(strip, carry):
        for copy in (across(strip), to_core(strip), relay(strip), send_far(strip)):
            copy.wait_send()
        keep_tile(strip).wait()
        in_core(strip).wait()
        in_relay(strip).wait()
        in_across(strip).wait_send()

        @pl.when(outer)
        def _():
            to_inner(strip, other, 0).wait_send()
            to_inner(strip, own, 1).wait_send()

        @pl.when(inner)
        def _():
            for copy in (to_middle(strip), final_across(strip), final_out(strip), final_pass(strip)):
                copy.wait_send()

        return carry

    lax.fori_loop(0, strips, finish_strip, 0)

    for copy in (send_scale(), send_tok()):
        copy.wait_send()
    for index in range(PASSES):
        for copy in (send_out(index), out_across(index), out_core(index), out_relay(index)):
            copy.wait_send()
    send_sum().wait_send()
    send_late().wait_send()


def gather_hidden(patch_size, tok, weight, rows, check_weight, in_bias, old_in, old_out):
    rep_count = lax.axis_size("rep")
    tokens, depth = tok.shape
    local = weight.shape[1]
    _, tile_rows, group_cols = old_in.shape
    width, half_rows = group_cols // STRIPS, depth // 2
    any_space = pl.BlockSpec(memory_space=pl.ANY)
    vmem = pl.BlockSpec(memory_space=pltpu.VMEM)
    strip_shape = (half_rows, width)
    units = 2 * rep_count * STRIPS // PAIR
    dma = pltpu.SemaphoreType.DMA
    f32, bf16 = jnp.float32, jnp.bfloat16
    return pl.pallas_call(
        functools.partial(gather_kernel, patch_size),
        out_shape=(
            jax.ShapeDtypeStruct((rep_count, tile_rows, group_cols), old_in.dtype),
            jax.ShapeDtypeStruct((rep_count,) + old_out.shape[1:], old_out.dtype),
            jax.ShapeDtypeStruct((tokens, 128), f32),
        ),
        in_specs=[vmem] * 5 + [any_space] * 2,
        out_specs=(any_space, any_space, vmem),
        scratch_shapes=[
            pltpu.VMEM((tokens, 128), f32),
            pltpu.VMEM((8, 128), f32),
            pltpu.VMEM((tokens, 128), bf16),
            pltpu.VMEM((ROWS - 1, tokens, 128), bf16),
            pltpu.VMEM((8, tokens), f32),
            pltpu.VMEM((ROWS - 1, 8, tokens), f32),
            pltpu.VMEM((local, 128), bf16),
            pltpu.VMEM((local, 128), bf16),
            pltpu.VMEM((tokens, tile_rows), bf16),
            pltpu.VMEM((tokens, tile_rows), bf16),
            pltpu.VMEM((rep_count,) + old_out.shape[1:], old_out.dtype),
            pltpu.VMEM((tokens, tile_rows), bf16),
            pltpu.VMEM((tokens, tile_rows), bf16),
            pltpu.VMEM((tokens, tile_rows), f32),
            pltpu.VMEM((tokens, tile_rows), f32),
            pltpu.VMEM((STRIPS, tile_rows, width), old_in.dtype),
            pltpu.VMEM((STRIPS, tile_rows, width), old_in.dtype),
            pltpu.VMEM((2, depth, tile_rows), bf16),
            pltpu.VMEM((tokens, local), f32),
            pltpu.VMEM((STRIPS, 2) + strip_shape, bf16),
            pltpu.VMEM((STRIPS, 2) + strip_shape, bf16),
            pltpu.VMEM((STRIPS,) + strip_shape, bf16),
            pltpu.VMEM((STRIPS,) + strip_shape, bf16),
            pltpu.VMEM((STRIPS,) + strip_shape, bf16),
            pltpu.VMEM((rep_count, STRIPS, depth, width), bf16),
            pltpu.VMEM((2, tokens, depth), bf16),
            pltpu.VMEM((2, tokens, 128), f32),
            pltpu.VMEM((units, tokens, PAIR * width), bf16),
            pltpu.VMEM((8, depth), f32),
            pltpu.VMEM((ROWS - 1, 8, depth), f32),
            pltpu.VMEM((8, tokens), f32),
            pltpu.VMEM((ROWS - 1, 8, tokens), f32),
            pltpu.VMEM((8, tokens), f32),
            pltpu.VMEM((8, tokens), f32),
            dma((STRIPS,)),
            dma((STRIPS,)),
            dma((ROWS - 1, 2)),
            dma((ROWS - 1, 2)),
            dma((2,)),
            dma((STRIPS, 2)),
            dma((2,)),
            dma((STRIPS, 2, 2)),
            dma((STRIPS, 2)),
            dma((STRIPS, 3, 2)),
            dma((STRIPS,)),
            dma((STRIPS, 2)),
            dma((STRIPS, 2)),
            dma((STRIPS, 2)),
            dma((PASSES, 2)),
            dma((PASSES, 2)),
            dma((PASSES, 2)),
            dma((PASSES, 2)),
            dma((rep_count,)),
            dma((2, 2)),
            dma((STRIPS, 3, 2)),
            dma((ROWS - 1, 2)),
            dma((ROWS - 1, 2)),
        ],
        compiler_params=pltpu.CompilerParams(
            collective_id=0, has_side_effects=True, vmem_limit_bytes=66_000_000
        ),
        cost_estimate=pl.CostEstimate(flops=10**10, bytes_accessed=10**8, transcendentals=0),
        name="gather_hidden",
    )(tok, weight, rows, check_weight, in_bias.reshape(-1, 1, PAIR * width), old_in, old_out)


def row_of(restore_id, table):
    return lax.dynamic_slice_in_dim(table, restore_id[0], 1, axis=0)[0]


def fast_device(
    patches,
    embed_weight,
    embed_bias,
    old_in,
    old_out,
    restore_id,
    norm_gains,
    in_biases,
    out_biases,
    final_gain,
    check_weight,
):
    col, rep = lax.axis_index("col"), lax.axis_index("rep")
    rep_count, row_count = lax.axis_size("rep"), lax.axis_size("row")
    tile_rows = old_in.shape[1]
    token_count, patch_size = patches.shape
    feature_count = embed_weight.shape[1] * row_count
    depth = -(-(patch_size + 1) // 32) * 32

    in_bias = row_of(restore_id, in_biases)
    rows = jnp.stack(
        (embed_bias, row_of(restore_id, norm_gains), final_gain, row_of(restore_id, out_biases))
    )
    tok = jnp.concatenate(
        (
            patches,
            jnp.ones((token_count, 1), patches.dtype),
            jnp.zeros((token_count, depth - patch_size - 1), patches.dtype),
        ),
        axis=1,
    )
    weight = jnp.pad(embed_weight, ((0, depth - patch_size), (0, 0)))
    in_tiles, out_tiles, check_logits = gather_hidden(
        patch_size, tok, weight, rows, check_weight, in_bias, old_in, old_out
    )
    return (place_tiles(old_in, in_tiles, 0), place_tiles(old_out, out_tiles, 1), check_logits)


def on_either(*args):
    old_in = args[3]
    shared = (
        lax.axis_size("col") == 2
        and lax.axis_size("rep") == 4
        and lax.axis_size("row") == ROWS
        and old_in.shape[0] == 2 * lax.axis_size("rep")
    )
    return fast_device(*args) if shared else on_device(*args)


def solution(mesh):
    placed = (
        P(("rep", "col"), None),
        P(None, "row"),
        P("row"),
        P(("row", "col"), None, None),
        P(("row", "col"), None, None),
        P(),
        P(None, "row"),
        P(None, "col"),
        P(None, "row"),
        P("row"),
        P("row", None),
    )
    return jax.shard_map(
        on_either,
        mesh=mesh,
        in_specs=placed,
        out_specs=(P("row", "col"), P("col", "row"), P(("rep", "col"), None)),
        check_vma=False,
    )
```
